32 devices in a mesh: lam: 16 (over z, x, core), atom: 2 (over y).
Axes of the slice: x: 2, y: 2, z: 4, core: 2. Of those that a mesh axis runs over, the one named last changes fastest.
Arguments:
- coords: float32 [16, 3, 16384], P('lam', None, 'atom'), may hold values from 0 to 1
- velocities: float32 [16, 3, 16384], P('lam', None, 'atom'), may hold values from -6 to 6
- coupling: float32 [16, 2, 16384], P('lam', None, 'atom'), may hold values from 0.2 to 1
- charges: float32 [16384], replicated, may hold values from -1.5 to 1.5
- types: int32 [16384], replicated, may hold values from 0 to 15
- type_sigma: float32 [16], replicated, may hold values from 0.25 to 0.4
- type_eps: float32 [16], replicated, may hold values from 0.1 to 1
- near_tiles: int32 [128, 5], P('atom'), may hold values from 0 to 127
- accept: int32 [16], replicated, may hold values from 0 to 1, as said below
Outputs:
- energies: float32 [16, 3], P('lam')
- forces: float32 [16, 3, 16384], P('lam', None, 'atom')
- new_coords: float32 [16, 3, 16384], P('lam', None, 'atom')
- new_velocities: float32 [16, 3, 16384], P('lam', None, 'atom')
The draws below stay inside these ranges and needn't reach their ends.
Inputs may be any that keep to these rules, and one draw needn't show every extreme that they name: accept[r] = 1 exchanges replicas r and r + 1 (modulo 16); no two consecutive entries around the cycle are both 1.
All inputs are finite; a program needn't handle non-finite values.
Results may differ from the reference program's by a relative error of at most 0.0003.
Values sent between devices are 32-bit elements; how exact they have to be, the bound alone decides.
A program may use at most 64 MiB of HBM per device.

```python
import math
from functools import partial
import jax
import jax.numpy as jnp
from jax import lax

TILE = 128
NEAR = 5
NTYPES = 16
REPLICAS = 16
ATOMS = 16384
TILES = 128


def draw_accept(key, part):
    coins = jax.random.randint(jax.random.fold_in(key, 11), (REPLICAS,), 0, 2)
    return (coins * (1 - jnp.roll(coins, 1))).astype(jnp.int32)


def touch_ends(drawn, own_key, smallest, high):
    extent = drawn.shape
    spot = [jax.random.randint(jax.random.fold_in(own_key, axis), (), 0, extent[axis]) for axis in range(len(extent))]
    drawn = drawn.at[tuple(spot)].set(smallest)
    longest = extent.index(max(extent))
    spot[longest] = (spot[longest] + 1) % extent[longest]
    return drawn.at[tuple(spot)].set(high)


def block_levels(key, dims, shards, low, high):
    level = 1.0
    for position, blocks in shards:
        steps = jax.random.uniform(jax.random.fold_in(jax.random.fold_in(key, 6), position), (blocks,), jnp.float32, low / len(shards), high / len(shards))
        level = level * jnp.repeat(jnp.exp(steps), dims[position] // blocks).reshape((-1,) + (1,) * (len(dims) - 1 - position))
    return level


def centred(stream_key, shape, scale, bound, split=(), held_as=jnp.bfloat16):
    factor_of = block_levels(stream_key, shape, split, -0.22, 0.18) if split else 1.0
    array = jax.random.normal(stream_key, shape, jnp.float32) * scale * factor_of
    return jnp.minimum(jnp.maximum(array, -bound), bound).astype(held_as)


def setup_inputs(seed: int = 0) -> dict:
    streams_of = jax.random.split(jax.random.key(seed), 10)
    coords = jnp.clip(1.0 * jax.random.uniform(streams_of[0], (REPLICAS, 3, ATOMS), jnp.float32) ** block_levels(streams_of[0], (REPLICAS, 3, ATOMS), ((0, 16), (2, 2)), -0.2, 0.2), 0.0, 1.0)
    velocities = centred(streams_of[1], (REPLICAS, 3, ATOMS), 1.0, 6.0, ((0, 16), (2, 2)), jnp.float32)
    coupling = jnp.clip(jnp.exp(math.log(1.0) - 1.609438 * jax.random.uniform(streams_of[2], (REPLICAS, 2, ATOMS), jnp.float32) ** block_levels(streams_of[2], (REPLICAS, 2, ATOMS), ((0, 16), (2, 2)), -0.2, 0.2)), 0.2, 1.0)
    charges = centred(streams_of[3], (ATOMS,), 0.3, 1.5, (), jnp.float32)
    types = touch_ends(jax.random.randint(streams_of[4], (ATOMS,), 0, NTYPES), jax.random.fold_in(streams_of[4], 1), 0, NTYPES - 1).astype(jnp.int32)
    type_sigma = jnp.clip(jnp.exp(jax.random.uniform(streams_of[5], (NTYPES,), jnp.float32, math.log(0.25), math.log(0.4))), 0.25, 0.4)
    type_eps = jnp.clip(jnp.exp(jax.random.uniform(streams_of[6], (NTYPES,), jnp.float32, math.log(0.1), math.log(1.0))), 0.1, 1.0)
    near_tiles = touch_ends(jax.random.randint(streams_of[7], (TILES, NEAR), 0, TILES), jax.random.fold_in(streams_of[7], 1), 0, TILES - 1).astype(jnp.int32)
    accept = draw_accept(jax.random.fold_in(streams_of[9], 71), 0)
    return dict(coords=coords, velocities=velocities, coupling=coupling, charges=charges, types=types, type_sigma=type_sigma, type_eps=type_eps, near_tiles=near_tiles, accept=accept)


DELTA_SOFT = 0.05

def atom_params(charges, types, type_sigma, type_eps, coupling_whole):
    levels = lax.broadcasted_iota(jnp.int32, (type_sigma.shape[0], types.shape[0]), 0)
    onehot = (levels == types[None, :]).astype(jnp.float32)
    table = jnp.stack([type_sigma, jnp.sqrt(type_eps)])
    looked = jnp.dot(table, onehot, precision=lax.Precision.HIGHEST)
    return jnp.stack([charges * coupling_whole[0], looked[1] * coupling_whole[1], looked[0]])

def pair_block(inputs, with_force):
    rows_pos, cols_pos, rows_par, cols_par, rows_idx, cols_idx = inputs
    delta = rows_pos[:, :, None, :, None] - cols_pos[:, :, :, None, :]
    squared = lax.optimization_barrier(jnp.sum(delta * delta, axis=0))
    charge_pair = rows_par[0][:, None, :, None] * cols_par[0][:, :, None, :]
    depth_pair = rows_par[1][:, None, :, None] * cols_par[1][:, :, None, :]
    sigma_pair = 0.5 * (rows_par[2][:, None, :, None] + cols_par[2][:, :, None, :])
    sigma_area = sigma_pair * sigma_pair
    pair_keep = (rows_idx[:, None, :, None] != cols_idx[:, :, None, :]).astype(jnp.float32)
    inverse = lax.rsqrt(squared + DELTA_SOFT)
    ratio = sigma_area / (squared + sigma_area)
    cubed = ratio * ratio * ratio
    energy_pair = charge_pair * inverse + 4.0 * depth_pair * (cubed * cubed - cubed)
    total = jnp.sum(energy_pair * pair_keep)
    if not with_force:
        return (total, jnp.zeros_like(rows_pos))
    slope = -0.5 * charge_pair * inverse * inverse * inverse - 4.0 * depth_pair * (6.0 * cubed * ratio * ratio - 3.0 * ratio * ratio) * ratio * ratio / sigma_area
    weight = -2.0 * slope * pair_keep
    force = lax.optimization_barrier(jnp.sum(weight[None] * delta, axis=(2, 4)))
    return (total, force)

def evaluate(own_rows, whole, params, first_row, tile_list, with_force):
    count = own_rows.shape[1]
    row_tiles = count // TILE
    group = math.gcd(row_tiles, 4)
    blocks = row_tiles // group
    listed = tile_list.shape[1]
    rows_pos = own_rows.reshape(3, blocks, group, TILE).transpose(1, 0, 2, 3)
    own_par = lax.dynamic_slice_in_dim(params, first_row, count, 1)
    rows_par = own_par.reshape(3, blocks, group, TILE).transpose(1, 0, 2, 3)
    cols_pos = whole.reshape(3, -1, TILE)[:, tile_list].reshape(3, blocks, group, listed, TILE).transpose(1, 0, 2, 3, 4)
    cols_par = params.reshape(3, -1, TILE)[:, tile_list].reshape(3, blocks, group, listed, TILE).transpose(1, 0, 2, 3, 4)
    rows_idx = (first_row + jnp.arange(count, dtype=jnp.int32)).reshape(blocks, group, TILE)
    cols_idx = (tile_list[:, :, None] * TILE + jnp.arange(TILE, dtype=jnp.int32)[None, None, :]).reshape(blocks, group, listed, TILE)
    totals, forces = lax.map(partial(pair_block, with_force=with_force), (rows_pos, cols_pos, rows_par, cols_par, rows_idx, cols_idx))
    return (jnp.sum(totals), forces.transpose(1, 0, 2, 3).reshape(3, count))

def reference(coords, velocities, coupling, charges, types, type_sigma, type_eps, near_tiles, accept):
    count = coords.shape[0]

    def replica_terms(index):
        params = atom_params(charges, types, type_sigma, type_eps, coupling[index])
        own_coords = coords[index]
        lower_coords = coords[(index + count - 1) % count]
        upper_coords = coords[(index + 1) % count]
        energy_own, force = evaluate(own_coords, own_coords, params, 0, near_tiles, True)
        energy_low, unused = evaluate(lower_coords, lower_coords, params, 0, near_tiles, False)
        energy_up, unused = evaluate(upper_coords, upper_coords, params, 0, near_tiles, False)
        return (jnp.stack([energy_own, energy_low, energy_up]), force)
    totals_all, forces = lax.map(replica_terms, jnp.arange(count, dtype=jnp.int32))
    scale = 0.5 / ATOMS
    energies = jnp.stack([totals_all[:, 0], jnp.roll(totals_all[:, 2], 1), jnp.roll(totals_all[:, 1], -1)], axis=1) * scale
    upper_flag = (accept == 1)[:, None, None]
    lower_flag = (jnp.roll(accept, 1) == 1)[:, None, None]
    new_coords = jnp.where(upper_flag, jnp.roll(coords, -1, axis=0), jnp.where(lower_flag, jnp.roll(coords, 1, axis=0), coords))
    new_velocities = jnp.where(upper_flag, jnp.roll(velocities, -1, axis=0), jnp.where(lower_flag, jnp.roll(velocities, 1, axis=0), velocities))
    return (energies, forces, new_coords, new_velocities)
```

```python
from functools import partial

import jax
import jax.numpy as jnp
from jax import lax
from jax.experimental import pallas as pl
from jax.experimental.pallas import tpu as pltpu
from jax.sharding import PartitionSpec as P

TILE = 128
DELTA_SOFT = 0.05
SUB = 8


def moved(x, lam_by, atom_by):
    cycle, parts = lax.axis_size("lam"), lax.axis_size("atom")
    pairs = []
    for r in range(cycle):
        for a in range(parts):
            source = ((r - lam_by) % cycle) * parts + (a + atom_by) % parts
            pairs.append((source, r * parts + a))
    return lax.ppermute(x, ("lam", "atom"), pairs)


def tiles_kernel(parts, listed, *refs):
    where_ref, near_ref, sigma_ref, eps_ref, charges_ref, types_ref = refs[:6]
    halves = refs[6 : 6 + 4 * parts]
    force_ref, energy_ref, cols, turned, packed = refs[6 + 4 * parts :]
    width = halves[0].shape[2]
    row_tiles = width // TILE
    part = where_ref[0]

    kinds = types_ref[...]
    radius = jnp.zeros(kinds.shape, jnp.float32)
    depth = jnp.zeros(kinds.shape, jnp.float32)
    for level in range(sigma_ref.shape[0]):
        here = kinds == level
        radius = jnp.where(here, sigma_ref[level], radius)
        depth = jnp.where(here, eps_ref[level], depth)
    cols[3:4, :] = 0.5 * radius
    depth = 2.0 * jnp.sqrt(depth)
    cols[5:6, :] = depth
    cols[10:16, :] = jnp.zeros((6, kinds.shape[1]), jnp.float32)
    for step in range(parts):
        start = pl.multiple_of(lax.rem(part + step, parts) * width, TILE)
        span = pl.ds(start, width)
        cols[0:3, span] = halves[step][0]
    base = cols[5:6, :]
    for h in range(3):
        for step in range(parts):
            start = pl.multiple_of(lax.rem(part + step, parts) * width, TILE)
            span = pl.ds(start, width)
            scales = halves[parts * (h + 1) + step]
            cols[4 + 2 * h : 6 + 2 * h, span] = scales[0]
        cols[4 + 2 * h : 5 + 2 * h, :] = cols[4 + 2 * h : 5 + 2 * h, :] * charges_ref[...]
        cols[5 + 2 * h : 6 + 2 * h, :] = cols[5 + 2 * h : 6 + 2 * h, :] * base

    lane = lax.broadcasted_iota(jnp.int32, (SUB, TILE), 1)
    first_tile = part * row_tiles

    def row_tile(t, carry):
        totals, selfs = carry
        own = first_tile + t
        own_span = pl.ds(pl.multiple_of(own * TILE, TILE), TILE)
        turned[...] = cols[:, own_span].T
        near = [near_ref[t, k] for k in range(listed)]
        spans = [pl.ds(pl.multiple_of(n * TILE, TILE), TILE) for n in near]
        twice = jnp.float32(0.0)
        for n in near:
            twice = twice + (n == own).astype(jnp.float32)
        own_charge = [cols[4 + 2 * h : 5 + 2 * h, own_span] for h in range(3)]
        selfs = tuple(s + twice * (q * q) for s, q in zip(selfs, own_charge))

        def row_block(b, totals):
            rows = turned[pl.ds(pl.multiple_of(b * SUB, SUB), SUB), :]
            xi, yi, zi, ri, qi, ei, qa, ea, qb, eb = [
                jnp.broadcast_to(rows[:, c : c + 1], (SUB, TILE)) for c in range(10)
            ]
            e6 = 6.0 * ei
            sums = [None] * 9

            def put(slot, value):
                sums[slot] = value if sums[slot] is None else sums[slot] + value

            for span in spans:
                def col(c):
                    return jnp.broadcast_to(cols[c : c + 1, span], (SUB, TILE))

                dx, dy, dz = xi - col(0), yi - col(1), zi - col(2)
                s = dx * dx + dy * dy + dz * dz
                inv = lax.rsqrt(s + DELTA_SOFT)
                g = ri + col(3)
                area = g * g
                root = lax.rsqrt(s + area)
                p = root * root
                x = area * p
                x3 = x * x * x
                low = x3 - 1.0
                lj = x3 * low
                charge = col(4) * inv
                put(0, charge)
                put(1, col(5) * lj)
                put(2, col(6) * inv)
                put(3, col(7) * lj)
                put(4, col(8) * inv)
                put(5, col(9) * lj)
                w = qi * (charge * (inv * inv)) + (e6 * col(5)) * ((x3 * p) * (x3 + low))
                put(6, w * dx)
                put(7, w * dy)
                put(8, w * dz)
            fx, fy, fz = [jnp.sum(v, axis=1, keepdims=True) for v in sums[6:9]]
            packed[pl.ds(pl.multiple_of(b * SUB, SUB), SUB), :] = jnp.where(
                lane == 0, fx, jnp.where(lane == 1, fy, fz)
            )
            return (
                totals[0] + (qi * sums[0] + ei * sums[1]),
                totals[1] + (qa * sums[2] + ea * sums[3]),
                totals[2] + (qb * sums[4] + eb * sums[5]),
            )

        totals = lax.fori_loop(0, TILE // SUB, row_block, totals)
        out_span = pl.ds(pl.multiple_of(t * TILE, TILE), TILE)
        force_ref[0, :, out_span] = packed[...].T[0:3]
        return totals, selfs

    zero = jnp.zeros((SUB, TILE), jnp.float32)
    none = jnp.zeros((1, TILE), jnp.float32)
    totals, selfs = lax.fori_loop(0, row_tiles, row_tile, ((zero,) * 3, (none,) * 3))
    soft = lax.rsqrt(jnp.full((1, TILE), DELTA_SOFT, jnp.float32))
    lane1 = lax.broadcasted_iota(jnp.int32, (1, TILE), 1)
    line = jnp.zeros((1, TILE), jnp.float32)
    for h in range(3):
        value = jnp.sum(jnp.sum(totals[h], axis=0, keepdims=True) - selfs[h] * soft)
        line = jnp.where(lane1 == h, value, line)
    energy_ref[...] = line


def per_device(
    coords, velocities, coupling, charges, types, type_sigma, type_eps, near_tiles, accept
):
    parts, width = lax.axis_size("atom"), coords.shape[2]
    atoms = parts * width
    part = lax.axis_index("atom")
    halves = [coords] + [moved(coords, 0, step) for step in range(1, parts)]
    for by in (0, 1, -1):
        for step in range(parts):
            halves.append(coupling if by == step == 0 else moved(coupling, by, step))
    lower_coords, lower_moving = moved(coords, 1, 0), moved(velocities, 1, 0)
    upper_coords, upper_moving = moved(coords, -1, 0), moved(velocities, -1, 0)

    smem = pl.BlockSpec(memory_space=pltpu.SMEM)
    vmem = pl.BlockSpec(memory_space=pltpu.VMEM)
    pairs = width * near_tiles.shape[1] * TILE
    force, line = pl.pallas_call(
        partial(tiles_kernel, parts, near_tiles.shape[1]),
        out_shape=(
            jax.ShapeDtypeStruct(coords.shape, jnp.float32),
            jax.ShapeDtypeStruct((1, TILE), jnp.float32),
        ),
        in_specs=[smem] * 4 + [vmem] * (2 + len(halves)),
        out_specs=(vmem, vmem),
        scratch_shapes=[
            pltpu.VMEM((16, atoms), jnp.float32),
            pltpu.VMEM((TILE, 16), jnp.float32),
            pltpu.VMEM((TILE, TILE), jnp.float32),
        ],
        cost_estimate=pl.CostEstimate(
            flops=50 * pairs, bytes_accessed=4 * 20 * atoms, transcendentals=2 * pairs
        ),
        name="tiles",
    )(
        part.reshape(1).astype(jnp.int32),
        near_tiles,
        type_sigma,
        type_eps,
        charges.reshape(1, atoms),
        types.reshape(1, atoms),
        *halves,
    )
    shares = jnp.stack([line[0, :3]] + [moved(line, 0, step)[0, :3] for step in range(1, parts)])
    total = shares[0]
    for step in range(1, parts):
        total = total + shares[step]
    if parts > 2:
        order = (jnp.arange(parts) - part) % parts
        total = jnp.sum(shares[order], axis=0)
    energies = (total * (0.5 / atoms))[None]

    replica, cycle = lax.axis_index("lam"), lax.axis_size("lam")
    up = accept[replica] == 1
    low = accept[(replica + cycle - 1) % cycle] == 1
    new_coords = jnp.where(up, upper_coords, jnp.where(low, lower_coords, coords))
    new_velocities = jnp.where(up, upper_moving, jnp.where(low, lower_moving, velocities))
    return (energies, force, new_coords, new_velocities)


def solution(mesh):
    split = P("lam", None, "atom")
    return jax.shard_map(
        per_device,
        mesh=mesh,
        in_specs=(split, split, split, P(), P(), P(), P(), P("atom", None), P()),
        out_specs=(P("lam", None), split, split, split),
        check_vma=False,
    )
```

```python
from functools import partial

import jax
import jax.numpy as jnp
from jax import lax
from jax.experimental import pallas as pl
from jax.experimental.pallas import tpu as pltpu
from jax.sharding import PartitionSpec as P

TILE = 128
DELTA_SOFT = 0.05
SUB = 8
DEPTH = 48


def moved(x, lam_by, atom_by):
    cycle, parts = lax.axis_size("lam"), lax.axis_size("atom")
    pairs = []
    for r in range(cycle):
        for a in range(parts):
            source = ((r - lam_by) % cycle) * parts + (a + atom_by) % parts
            pairs.append((source, r * parts + a))
    return lax.ppermute(x, ("lam", "atom"), pairs)


def split3(x):
    high = x.astype(jnp.bfloat16).astype(jnp.float32)
    rest = x - high
    mid = rest.astype(jnp.bfloat16).astype(jnp.float32)
    return high, mid, rest - mid


def tiles_kernel(parts, listed, *refs):
    where_ref, near_ref, sigma_ref, eps_ref, charges_ref, types_ref = refs[:6]
    halves = refs[6 : 6 + 4 * parts]
    force_ref, energy_ref, cols, left, right, lbuf, rbuf = refs[6 + 4 * parts : 13 + 4 * parts]
    geos, turns, packs = [refs[13 + 4 * parts + 2 * i :][:2] for i in range(3)]
    width = halves[0].shape[2]
    atoms = cols.shape[1]
    row_tiles = width // TILE
    part = where_ref[0]
    first_tile = part * row_tiles

    kinds = types_ref[...]
    radius = jnp.zeros(kinds.shape, jnp.float32)
    depth = jnp.zeros(kinds.shape, jnp.float32)
    for level in range(sigma_ref.shape[0]):
        here = kinds == level
        radius = jnp.where(here, sigma_ref[level], radius)
        depth = jnp.where(here, eps_ref[level], depth)
    cols[3:4, :] = 0.5 * radius
    cols[10:16, :] = jnp.zeros((6, atoms), jnp.float32)
    base = 2.0 * jnp.sqrt(depth)
    spans = []
    for step in range(parts):
        start = pl.multiple_of(lax.rem(part + step, parts) * width, TILE)
        spans.append(pl.ds(start, width))
        cols[0:3, spans[step]] = halves[step][0] - 0.5
    for h in range(3):
        for step in range(parts):
            cols[4 + 2 * h : 6 + 2 * h, spans[step]] = halves[parts * (h + 1) + step][0]
        cols[4 + 2 * h : 5 + 2 * h, :] = cols[4 + 2 * h : 5 + 2 * h, :] * charges_ref[...]
        cols[5 + 2 * h : 6 + 2 * h, :] = cols[5 + 2 * h : 6 + 2 * h, :] * base

    chunk = lbuf.shape[1]
    lbuf[...] = jnp.zeros(lbuf.shape, jnp.float32)
    rbuf[...] = jnp.zeros(rbuf.shape, jnp.float32)
    lbuf[30:39, :] = jnp.ones((9, chunk), jnp.float32)
    rbuf[24:30, :] = jnp.ones((6, chunk), jnp.float32)
    soft_parts = split3(jnp.full((1, chunk), DELTA_SOFT, jnp.float32))
    for i in range(3):
        rbuf[36 + i : 37 + i, :] = soft_parts[i]
    row = lax.broadcasted_iota(jnp.int32, (DEPTH, TILE), 0)
    cross = row < 24
    radial = cross & (lax.rem(row, 4) == 3) | ((row >= 27) & (row < 30)) | ((row >= 33) & (row < 36))
    keep_u = (~radial) & (row < 39)
    keep_v = row < 36
    keeps = (keep_u, keep_v, radial)
    quad = lax.broadcasted_iota(jnp.int32, (4, chunk), 0)
    sign = jnp.where(quad == 3, 2.0, -2.0).astype(jnp.float32)

    def prepare(c, carry):
        span = pl.ds(pl.multiple_of(c * chunk, TILE), chunk)
        four = cols[0:4, span]
        square = four * four
        norm = split3(square[0:1] + square[1:2] + square[2:3])
        area = split3(square[3:4])
        high, mid, low = split3(four)
        shigh, smid, slow = high * sign, mid * sign, low * sign
        for i, v in enumerate((high, high, mid, mid, high, low)):
            lbuf[4 * i : 4 * i + 4, :] = v
        for i, v in enumerate((shigh, smid, shigh, smid, slow, shigh)):
            rbuf[4 * i : 4 * i + 4, :] = v
        for i in range(3):
            lbuf[24 + i : 25 + i, :] = norm[i]
            lbuf[27 + i : 28 + i, :] = area[i]
            rbuf[30 + i : 31 + i, :] = norm[i]
            rbuf[33 + i : 34 + i, :] = area[i]
        lbuf[40:41, :] = cols[4:5, span]
        lbuf[41:42, :] = 6.0 * cols[5:6, span]
        left[:, span] = lbuf[...]
        for i in range(chunk // TILE):
            block = rbuf[:, i * TILE : (i + 1) * TILE]
            for j in range(3):
                place = pl.multiple_of((c * (chunk // TILE) + i) * (3 * TILE) + j * TILE, TILE)
                right[:, pl.ds(place, TILE)] = jnp.where(keeps[j], block, 0.0).astype(jnp.bfloat16)
        return carry

    lax.fori_loop(0, atoms // chunk, prepare, 0)

    lane = lax.broadcasted_iota(jnp.int32, (SUB, TILE), 1)

    def geometry(t, s):
        own_span = pl.ds(pl.multiple_of((first_tile + t) * TILE, TILE), TILE)
        turned = left[:, own_span].T
        turns[s][...] = turned
        lhs = turned.astype(jnp.bfloat16)
        for k in range(listed):
            span = pl.ds(pl.multiple_of(near_ref[t, k] * (3 * TILE), TILE), 3 * TILE)
            geos[s][k] = jnp.dot(lhs, right[:, span], preferred_element_type=jnp.float32)

    def blocks(t, s, selfs):
        own = first_tile + t
        own_span = pl.ds(pl.multiple_of(own * TILE, TILE), TILE)
        near = [near_ref[t, k] for k in range(listed)]
        near_spans = [pl.ds(pl.multiple_of(n * TILE, TILE), TILE) for n in near]
        twice = jnp.float32(0.0)
        for n in near:
            twice = twice + (n == own).astype(jnp.float32)
        mine = cols[:, own_span]
        selfs = selfs + twice * (mine * mine)
        for b in range(TILE // SUB):
            rows = pl.ds(b * SUB, SUB)
            qi = jnp.broadcast_to(turns[s][rows, 40:41], (SUB, TILE))
            e6 = jnp.broadcast_to(turns[s][rows, 41:42], (SUB, TILE))
            sums = [None] * 10

            def put(slot, value):
                sums[slot] = value if sums[slot] is None else sums[slot] + value

            for k, span in enumerate(near_spans):
                def col(c):
                    return jnp.broadcast_to(cols[c : c + 1, span], (SUB, TILE))

                inv = lax.rsqrt(geos[s][k, rows, 0:TILE])
                root = lax.rsqrt(geos[s][k, rows, TILE : 2 * TILE])
                p = root * root
                x = geos[s][k, rows, 2 * TILE : 3 * TILE] * p
                x3 = x * x * x
                low = x3 - 1.0
                lj = x3 * low
                charge = col(4) * inv
                put(4, charge)
                put(5, col(5) * lj)
                put(6, col(6) * inv)
                put(7, col(7) * lj)
                put(8, col(8) * inv)
                put(9, col(9) * lj)
                w = qi * (charge * (inv * inv)) + (e6 * col(5)) * ((x3 * p) * (x3 + low))
                put(0, w * col(0))
                put(1, w * col(1))
                put(2, w * col(2))
                put(3, w)
            line = jnp.sum(sums[9], axis=1, keepdims=True)
            for c in range(8, -1, -1):
                line = jnp.where(lane == c, jnp.sum(sums[c], axis=1, keepdims=True), line)
            packs[s][rows, :] = line
        return selfs

    def finish(t, s, totals):
        own_span = pl.ds(pl.multiple_of((first_tile + t) * TILE, TILE), TILE)
        flat = packs[s][...].T[0:16]
        mine = cols[:, own_span]
        out_span = pl.ds(pl.multiple_of(t * TILE, TILE), TILE)
        force_ref[0, :, out_span] = mine[0:3] * flat[3:4] - flat[0:3]
        return totals + mine * flat

    def two_tiles(m, carry):
        totals, selfs = carry
        t = 2 * m
        totals = finish(jnp.maximum(t - 1, 0), 1, totals)
        geometry(t + 1, 1)
        selfs = blocks(t, 0, selfs)
        totals = finish(t, 0, totals)
        geometry(jnp.minimum(t + 2, row_tiles - 1), 0)
        selfs = blocks(t + 1, 1, selfs)
        return totals, selfs

    zero = jnp.zeros((16, TILE), jnp.float32)
    packs[1][...] = jnp.zeros(packs[1].shape, jnp.float32)
    geometry(0, 0)
    totals, selfs = lax.fori_loop(0, row_tiles // 2, two_tiles, (zero, zero))
    totals = finish(row_tiles - 1, 1, totals)
    soft = lax.rsqrt(jnp.full((1, TILE), DELTA_SOFT, jnp.float32))
    lane1 = lax.broadcasted_iota(jnp.int32, (1, TILE), 1)
    line = jnp.zeros((1, TILE), jnp.float32)
    for h in range(3):
        c = 4 + 2 * h
        value = jnp.sum(totals[c : c + 1] + totals[c + 1 : c + 2] - selfs[c : c + 1] * soft)
        line = jnp.where(lane1 == h, value, line)
    energy_ref[...] = line


def per_device(
    coords, velocities, coupling, charges, types, type_sigma, type_eps, near_tiles, accept
):
    parts, width = lax.axis_size("atom"), coords.shape[2]
    atoms = parts * width
    part = lax.axis_index("atom")
    halves = [coords] + [moved(coords, 0, step) for step in range(1, parts)]
    for by in (0, 1, -1):
        for step in range(parts):
            halves.append(coupling if by == step == 0 else moved(coupling, by, step))
    lower_coords, lower_moving = moved(coords, 1, 0), moved(velocities, 1, 0)
    upper_coords, upper_moving = moved(coords, -1, 0), moved(velocities, -1, 0)

    smem = pl.BlockSpec(memory_space=pltpu.SMEM)
    vmem = pl.BlockSpec(memory_space=pltpu.VMEM)
    pairs = width * near_tiles.shape[1] * TILE
    force, line = pl.pallas_call(
        partial(tiles_kernel, parts, near_tiles.shape[1]),
        out_shape=(
            jax.ShapeDtypeStruct(coords.shape, jnp.float32),
            jax.ShapeDtypeStruct((1, TILE), jnp.float32),
        ),
        in_specs=[smem] * 4 + [vmem] * (2 + len(halves)),
        out_specs=(vmem, vmem),
        scratch_shapes=[
            pltpu.VMEM((16, atoms), jnp.float32),
            pltpu.VMEM((DEPTH, atoms), jnp.float32),
            pltpu.VMEM((DEPTH, 3 * atoms), jnp.bfloat16),
            pltpu.VMEM((DEPTH, 4 * TILE), jnp.float32),
            pltpu.VMEM((DEPTH, 4 * TILE), jnp.float32),
        ]
        + [pltpu.VMEM((near_tiles.shape[1], TILE, 3 * TILE), jnp.float32)] * 2
        + [pltpu.VMEM((TILE, DEPTH), jnp.float32)] * 2
        + [pltpu.VMEM((TILE, TILE), jnp.float32)] * 2,
        cost_estimate=pl.CostEstimate(
            flops=50 * pairs, bytes_accessed=4 * 20 * atoms, transcendentals=2 * pairs
        ),
        name="tiles",
    )(
        part.reshape(1).astype(jnp.int32),
        near_tiles,
        type_sigma,
        type_eps,
        charges.reshape(1, atoms),
        types.reshape(1, atoms),
        *halves,
    )
    shares = jnp.stack([line[0, :3]] + [moved(line, 0, step)[0, :3] for step in range(1, parts)])
    total = shares[0]
    for step in range(1, parts):
        total = total + shares[step]
    if parts > 2:
        order = (jnp.arange(parts) - part) % parts
        total = jnp.sum(shares[order], axis=0)
    energies = (total * (0.5 / atoms))[None]

    replica, cycle = lax.axis_index("lam"), lax.axis_size("lam")
    up = accept[replica] == 1
    low = accept[(replica + cycle - 1) % cycle] == 1
    new_coords = jnp.where(up, upper_coords, jnp.where(low, lower_coords, coords))
    new_velocities = jnp.where(up, upper_moving, jnp.where(low, lower_moving, velocities))
    return (energies, force, new_coords, new_velocities)


def solution(mesh):
    split = P("lam", None, "atom")
    return jax.shard_map(
        per_device,
        mesh=mesh,
        in_specs=(split, split, split, P(), P(), P(), P(), P("atom", None), P()),
        out_specs=(P("lam", None), split, split, split),
        check_vma=False,
    )
```

```python
from functools import partial

import jax
import jax.numpy as jnp
from jax import lax
from jax.experimental import pallas as pl
from jax.experimental.pallas import tpu as pltpu
from jax.sharding import PartitionSpec as P

TILE = 128
DELTA_SOFT = 0.05
SUB = 8
DEPTH = 48


def moved(x, lam_by, atom_by):
    cycle, parts = lax.axis_size("lam"), lax.axis_size("atom")
    pairs = []
    for r in range(cycle):
        for a in range(parts):
            source = ((r - lam_by) % cycle) * parts + (a + atom_by) % parts
            pairs.append((source, r * parts + a))
    return lax.ppermute(x, ("lam", "atom"), pairs)


def split3(x):
    high = x.astype(jnp.bfloat16).astype(jnp.float32)
    rest = x - high
    mid = rest.astype(jnp.bfloat16).astype(jnp.float32)
    return high, mid, rest - mid


def lane_sums(ones, x):
    return lax.dot_general(
        ones, x, (((1,), (1,)), ((), ())), preferred_element_type=jnp.float32
    )


def tiles_kernel(parts, listed, *refs):
    where_ref, near_ref, sigma_ref, eps_ref, charges_ref, types_ref = refs[:6]
    halves = refs[6 : 6 + 4 * parts]
    force_ref, energy_ref, cols, left, right, lbuf, rbuf = refs[6 + 4 * parts : 13 + 4 * parts]
    geos, owns, accs = [refs[13 + 4 * parts + 2 * i :][:2] for i in range(3)]
    width = halves[0].shape[2]
    atoms = cols.shape[1]
    row_tiles = width // TILE
    part = where_ref[0]
    first_tile = part * row_tiles

    kinds = types_ref[...]
    radius = jnp.zeros(kinds.shape, jnp.float32)
    depth = jnp.zeros(kinds.shape, jnp.float32)
    for level in range(sigma_ref.shape[0]):
        here = kinds == level
        radius = jnp.where(here, sigma_ref[level], radius)
        depth = jnp.where(here, eps_ref[level], depth)
    cols[3:4, :] = 0.5 * radius
    cols[10:16, :] = jnp.zeros((6, atoms), jnp.float32)
    base = 2.0 * jnp.sqrt(depth)
    spans = []
    for step in range(parts):
        start = pl.multiple_of(lax.rem(part + step, parts) * width, TILE)
        spans.append(pl.ds(start, width))
        cols[0:3, spans[step]] = halves[step][0] - 0.5
    for h in range(3):
        for step in range(parts):
            cols[4 + 2 * h : 6 + 2 * h, spans[step]] = halves[parts * (h + 1) + step][0]
        cols[4 + 2 * h : 5 + 2 * h, :] = cols[4 + 2 * h : 5 + 2 * h, :] * charges_ref[...]
        cols[5 + 2 * h : 6 + 2 * h, :] = cols[5 + 2 * h : 6 + 2 * h, :] * base

    chunk = lbuf.shape[1]
    lbuf[...] = jnp.zeros(lbuf.shape, jnp.float32)
    rbuf[...] = jnp.zeros(rbuf.shape, jnp.float32)
    lbuf[30:39, :] = jnp.ones((9, chunk), jnp.float32)
    rbuf[24:30, :] = jnp.ones((6, chunk), jnp.float32)
    soft_parts = split3(jnp.full((1, chunk), DELTA_SOFT, jnp.float32))
    for i in range(3):
        rbuf[36 + i : 37 + i, :] = soft_parts[i]
    row = lax.broadcasted_iota(jnp.int32, (DEPTH, TILE), 0)
    cross = row < 24
    radial = cross & (lax.rem(row, 4) == 3) | ((row >= 27) & (row < 30)) | ((row >= 33) & (row < 36))
    keep_u = (~radial) & (row < 39)
    keep_v = row < 36
    keeps = (keep_u, keep_v, radial)
    quad = lax.broadcasted_iota(jnp.int32, (4, chunk), 0)
    sign = jnp.where(quad == 3, 2.0, -2.0).astype(jnp.float32)

    def prepare(c, carry):
        span = pl.ds(pl.multiple_of(c * chunk, TILE), chunk)
        four = cols[0:4, span]
        square = four * four
        norm = split3(square[0:1] + square[1:2] + square[2:3])
        area = split3(square[3:4])
        high, mid, low = split3(four)
        shigh, smid, slow = high * sign, mid * sign, low * sign
        for i, v in enumerate((high, high, mid, mid, high, low)):
            lbuf[4 * i : 4 * i + 4, :] = v
        for i, v in enumerate((shigh, smid, shigh, smid, slow, shigh)):
            rbuf[4 * i : 4 * i + 4, :] = v
        for i in range(3):
            lbuf[24 + i : 25 + i, :] = norm[i]
            lbuf[27 + i : 28 + i, :] = area[i]
            rbuf[30 + i : 31 + i, :] = norm[i]
            rbuf[33 + i : 34 + i, :] = area[i]
        charge = split3(cols[4:5, span])
        well = split3(6.0 * cols[5:6, span])
        for i in range(3):
            lbuf[40 + i : 41 + i, :] = charge[i]
            lbuf[43 + i : 44 + i, :] = well[i]
        left[:, span] = lbuf[...]
        for i in range(chunk // TILE):
            block = rbuf[:, i * TILE : (i + 1) * TILE]
            for j in range(3):
                place = pl.multiple_of((c * (chunk // TILE) + i) * (3 * TILE) + j * TILE, TILE)
                right[:, pl.ds(place, TILE)] = jnp.where(keeps[j], block, 0.0).astype(jnp.bfloat16)
        return carry

    lax.fori_loop(0, atoms // chunk, prepare, 0)

    side = lax.broadcasted_iota(jnp.int32, (DEPTH, 2 * TILE), 1) < TILE
    deep = lax.broadcasted_iota(jnp.int32, (DEPTH, 2 * TILE), 0)
    spread = jnp.where(
        side & (deep >= 40) & (deep < 43) | (~side) & (deep >= 43) & (deep < 46), 1.0, 0.0
    ).astype(jnp.bfloat16)
    ones = jnp.ones((SUB, TILE), jnp.bfloat16)

    def geometry(t, s):
        own_span = pl.ds(pl.multiple_of((first_tile + t) * TILE, TILE), TILE)
        lhs = left[:, own_span].T.astype(jnp.bfloat16)
        owns[s][...] = jnp.dot(lhs, spread, preferred_element_type=jnp.float32)
        for k in range(listed):
            span = pl.ds(pl.multiple_of(near_ref[t, k] * (3 * TILE), TILE), 3 * TILE)
            geos[s][k] = jnp.dot(lhs, right[:, span], preferred_element_type=jnp.float32)

    def blocks(t, s, selfs):
        own = first_tile + t
        own_span = pl.ds(pl.multiple_of(own * TILE, TILE), TILE)
        near = [near_ref[t, k] for k in range(listed)]
        near_spans = [pl.ds(pl.multiple_of(n * TILE, TILE), TILE) for n in near]
        twice = jnp.float32(0.0)
        for n in near:
            twice = twice + (n == own).astype(jnp.float32)
        mine = cols[:, own_span]
        selfs = selfs + twice * (mine * mine)
        for b in range(TILE // SUB):
            rows = pl.ds(b * SUB, SUB)
            qi = owns[s][rows, 0:TILE]
            e6 = owns[s][rows, TILE : 2 * TILE]
            sums = [None] * 10

            def put(slot, value):
                sums[slot] = value if sums[slot] is None else sums[slot] + value

            for k, span in enumerate(near_spans):
                def col(c):
                    return jnp.broadcast_to(cols[c : c + 1, span], (SUB, TILE))

                inv = lax.rsqrt(geos[s][k, rows, 0:TILE])
                root = lax.rsqrt(geos[s][k, rows, TILE : 2 * TILE])
                p = root * root
                x = geos[s][k, rows, 2 * TILE : 3 * TILE] * p
                x3 = x * x * x
                low = x3 - 1.0
                lj = x3 * low
                charge = col(4) * inv
                put(4, charge)
                put(5, col(5) * lj)
                put(6, col(6) * inv)
                put(7, col(7) * lj)
                put(8, col(8) * inv)
                put(9, col(9) * lj)
                w = qi * (charge * (inv * inv)) + (e6 * col(5)) * ((x3 * p) * (x3 + low))
                put(0, w * col(0))
                put(1, w * col(1))
                put(2, w * col(2))
                put(3, w)
            for c in range(10):
                accs[s][c, rows, :] = sums[c]
        return selfs

    def finish(t, s, totals):
        own_span = pl.ds(pl.multiple_of((first_tile + t) * TILE, TILE), TILE)
        flat = []
        for c in range(10):
            whole = accs[s][c]
            high = whole.astype(jnp.bfloat16)
            rest = (whole - high.astype(jnp.float32)).astype(jnp.bfloat16)
            flat.append(lane_sums(ones, high)[0:1] + lane_sums(ones, rest)[0:1])
        mine = cols[:, own_span]
        out_span = pl.ds(pl.multiple_of(t * TILE, TILE), TILE)
        for c in range(3):
            force_ref[0, c : c + 1, out_span] = mine[c : c + 1] * flat[3] - flat[c]
        return tuple(
            totals[h]
            + (mine[4 + 2 * h : 5 + 2 * h] * flat[4 + 2 * h] + mine[5 + 2 * h : 6 + 2 * h] * flat[5 + 2 * h])
            for h in range(3)
        )

    def two_tiles(m, carry):
        totals, selfs = carry
        t = 2 * m
        totals = finish(jnp.maximum(t - 1, 0), 1, totals)
        geometry(t + 1, 1)
        selfs = blocks(t, 0, selfs)
        totals = finish(t, 0, totals)
        geometry(jnp.minimum(t + 2, row_tiles - 1), 0)
        selfs = blocks(t + 1, 1, selfs)
        return totals, selfs

    zero = jnp.zeros((16, TILE), jnp.float32)
    none = jnp.zeros((1, TILE), jnp.float32)
    accs[1][...] = jnp.zeros(accs[1].shape, jnp.float32)
    geometry(0, 0)
    totals, selfs = lax.fori_loop(0, row_tiles // 2, two_tiles, ((none,) * 3, zero))
    totals = finish(row_tiles - 1, 1, totals)
    soft = lax.rsqrt(jnp.full((1, TILE), DELTA_SOFT, jnp.float32))
    lane1 = lax.broadcasted_iota(jnp.int32, (1, TILE), 1)
    line = jnp.zeros((1, TILE), jnp.float32)
    for h in range(3):
        c = 4 + 2 * h
        value = jnp.sum(totals[h] - selfs[c : c + 1] * soft)
        line = jnp.where(lane1 == h, value, line)
    energy_ref[...] = line


def per_device(
    coords, velocities, coupling, charges, types, type_sigma, type_eps, near_tiles, accept
):
    parts, width = lax.axis_size("atom"), coords.shape[2]
    atoms = parts * width
    part = lax.axis_index("atom")
    halves = [coords] + [moved(coords, 0, step) for step in range(1, parts)]
    for by in (0, 1, -1):
        for step in range(parts):
            halves.append(coupling if by == step == 0 else moved(coupling, by, step))
    lower_coords, lower_moving = moved(coords, 1, 0), moved(velocities, 1, 0)
    upper_coords, upper_moving = moved(coords, -1, 0), moved(velocities, -1, 0)

    smem = pl.BlockSpec(memory_space=pltpu.SMEM)
    vmem = pl.BlockSpec(memory_space=pltpu.VMEM)
    pairs = width * near_tiles.shape[1] * TILE
    force, line = pl.pallas_call(
        partial(tiles_kernel, parts, near_tiles.shape[1]),
        out_shape=(
            jax.ShapeDtypeStruct(coords.shape, jnp.float32),
            jax.ShapeDtypeStruct((1, TILE), jnp.float32),
        ),
        in_specs=[smem] * 4 + [vmem] * (2 + len(halves)),
        out_specs=(vmem, vmem),
        scratch_shapes=[
            pltpu.VMEM((16, atoms), jnp.float32),
            pltpu.VMEM((DEPTH, atoms), jnp.float32),
            pltpu.VMEM((DEPTH, 3 * atoms), jnp.bfloat16),
            pltpu.VMEM((DEPTH, 4 * TILE), jnp.float32),
            pltpu.VMEM((DEPTH, 4 * TILE), jnp.float32),
        ]
        + [pltpu.VMEM((near_tiles.shape[1], TILE, 3 * TILE), jnp.float32)] * 2
        + [pltpu.VMEM((TILE, 2 * TILE), jnp.float32)] * 2
        + [pltpu.VMEM((10, TILE, TILE), jnp.float32)] * 2,
        cost_estimate=pl.CostEstimate(
            flops=50 * pairs, bytes_accessed=4 * 20 * atoms, transcendentals=2 * pairs
        ),
        name="tiles",
    )(
        part.reshape(1).astype(jnp.int32),
        near_tiles,
        type_sigma,
        type_eps,
        charges.reshape(1, atoms),
        types.reshape(1, atoms),
        *halves,
    )
    shares = jnp.stack([line[0, :3]] + [moved(line, 0, step)[0, :3] for step in range(1, parts)])
    total = shares[0]
    for step in range(1, parts):
        total = total + shares[step]
    if parts > 2:
        order = (jnp.arange(parts) - part) % parts
        total = jnp.sum(shares[order], axis=0)
    energies = (total * (0.5 / atoms))[None]

    replica, cycle = lax.axis_index("lam"), lax.axis_size("lam")
    up = accept[replica] == 1
    low = accept[(replica + cycle - 1) % cycle] == 1
    new_coords = jnp.where(up, upper_coords, jnp.where(low, lower_coords, coords))
    new_velocities = jnp.where(up, upper_moving, jnp.where(low, lower_moving, velocities))
    return (energies, force, new_coords, new_velocities)


def solution(mesh):
    split = P("lam", None, "atom")
    return jax.shard_map(
        per_device,
        mesh=mesh,
        in_specs=(split, split, split, P(), P(), P(), P(), P("atom", None), P()),
        out_specs=(P("lam", None), split, split, split),
        check_vma=False,
    )
```

```python
from functools import partial

import jax
import jax.numpy as jnp
from jax import lax
from jax.experimental import pallas as pl
from jax.experimental.pallas import tpu as pltpu
from jax.sharding import PartitionSpec as P

TILE = 128
DELTA_SOFT = 0.05
SUB = 8
DEPTH = 48


def moved(x, lam_by, atom_by):
    cycle, parts = lax.axis_size("lam"), lax.axis_size("atom")
    pairs = []
    for r in range(cycle):
        for a in range(parts):
            source = ((r - lam_by) % cycle) * parts + (a + atom_by) % parts
            pairs.append((source, r * parts + a))
    return lax.ppermute(x, ("lam", "atom"), pairs)


def split3(x):
    high = x.astype(jnp.bfloat16).astype(jnp.float32)
    rest = x - high
    mid = rest.astype(jnp.bfloat16).astype(jnp.float32)
    return high, mid, rest - mid


def lane_sums(ones, x):
    return lax.dot_general(
        ones, x, (((1,), (1,)), ((), ())), preferred_element_type=jnp.float32
    )


def tiles_kernel(parts, listed, *refs):
    where_ref, near_ref, sigma_ref, eps_ref, charges_ref, types_ref = refs[:6]
    halves = refs[6 : 6 + 3 * parts]
    force_ref, energy_ref, cols, left, right, lbuf, rbuf = refs[6 + 3 * parts : 13 + 3 * parts]
    geos, owns, accs = [refs[13 + 3 * parts + 2 * i :][:2] for i in range(3)]
    width = halves[0].shape[2]
    atoms = cols.shape[1]
    row_tiles = width // TILE
    part = where_ref[0]
    first_tile = part * row_tiles

    kinds = types_ref[...]
    radius = jnp.zeros(kinds.shape, jnp.float32)
    depth = jnp.zeros(kinds.shape, jnp.float32)
    for level in range(sigma_ref.shape[0]):
        here = kinds == level
        radius = jnp.where(here, sigma_ref[level], radius)
        depth = jnp.where(here, eps_ref[level], depth)
    cols[3:4, :] = 0.5 * radius
    cols[10:16, :] = jnp.zeros((6, atoms), jnp.float32)
    base = 2.0 * jnp.sqrt(depth)
    spans = []
    for step in range(parts):
        start = pl.multiple_of(lax.rem(part + step, parts) * width, TILE)
        spans.append(pl.ds(start, width))
        cols[0:3, spans[step]] = halves[step][0, 0:3] - 0.5
    for h in range(3):
        for step in range(parts):
            block = halves[parts * h + step]
            last = block.shape[1]
            cols[4 + 2 * h : 6 + 2 * h, spans[step]] = block[0, last - 2 : last]
        cols[4 + 2 * h : 5 + 2 * h, :] = cols[4 + 2 * h : 5 + 2 * h, :] * charges_ref[...]
        cols[5 + 2 * h : 6 + 2 * h, :] = cols[5 + 2 * h : 6 + 2 * h, :] * base

    chunk = lbuf.shape[1]
    lbuf[...] = jnp.zeros(lbuf.shape, jnp.float32)
    rbuf[...] = jnp.zeros(rbuf.shape, jnp.float32)
    lbuf[30:39, :] = jnp.ones((9, chunk), jnp.float32)
    rbuf[24:30, :] = jnp.ones((6, chunk), jnp.float32)
    soft_parts = split3(jnp.full((1, chunk), DELTA_SOFT, jnp.float32))
    for i in range(3):
        rbuf[36 + i : 37 + i, :] = soft_parts[i]
    row = lax.broadcasted_iota(jnp.int32, (DEPTH, TILE), 0)
    cross = row < 24
    radial = cross & (lax.rem(row, 4) == 3) | ((row >= 27) & (row < 30)) | ((row >= 33) & (row < 36))
    keep_u = (~radial) & (row < 39)
    keep_v = row < 36
    keeps = (keep_u, keep_v, radial)
    quad = lax.broadcasted_iota(jnp.int32, (4, chunk), 0)
    sign = jnp.where(quad == 3, 2.0, -2.0).astype(jnp.float32)

    def prepare(c, carry):
        span = pl.ds(pl.multiple_of(c * chunk, TILE), chunk)
        four = cols[0:4, span]
        square = four * four
        norm = split3(square[0:1] + square[1:2] + square[2:3])
        area = split3(square[3:4])
        high, mid, low = split3(four)
        shigh, smid, slow = high * sign, mid * sign, low * sign
        for i, v in enumerate((high, high, mid, mid, high, low)):
            lbuf[4 * i : 4 * i + 4, :] = v
        for i, v in enumerate((shigh, smid, shigh, smid, slow, shigh)):
            rbuf[4 * i : 4 * i + 4, :] = v
        for i in range(3):
            lbuf[24 + i : 25 + i, :] = norm[i]
            lbuf[27 + i : 28 + i, :] = area[i]
            rbuf[30 + i : 31 + i, :] = norm[i]
            rbuf[33 + i : 34 + i, :] = area[i]
        charge = split3(cols[4:5, span])
        well = split3(6.0 * cols[5:6, span])
        for i in range(3):
            lbuf[40 + i : 41 + i, :] = charge[i]
            lbuf[43 + i : 44 + i, :] = well[i]
        left[:, span] = lbuf[...]
        for i in range(chunk // TILE):
            block = rbuf[:, i * TILE : (i + 1) * TILE]
            for j in range(3):
                place = pl.multiple_of((c * (chunk // TILE) + i) * (3 * TILE) + j * TILE, TILE)
                right[:, pl.ds(place, TILE)] = jnp.where(keeps[j], block, 0.0).astype(jnp.bfloat16)
        return carry

    lax.fori_loop(0, atoms // chunk, prepare, 0)

    side = lax.broadcasted_iota(jnp.int32, (DEPTH, 2 * TILE), 1) < TILE
    deep = lax.broadcasted_iota(jnp.int32, (DEPTH, 2 * TILE), 0)
    spread = jnp.where(
        side & (deep >= 40) & (deep < 43) | (~side) & (deep >= 43) & (deep < 46), 1.0, 0.0
    ).astype(jnp.bfloat16)
    ones = jnp.ones((SUB, 2 * TILE), jnp.bfloat16)

    def geometry(t, s):
        own_span = pl.ds(pl.multiple_of((first_tile + t) * TILE, TILE), TILE)
        lhs = left[:, own_span].T.astype(jnp.bfloat16)
        owns[s][...] = jnp.dot(lhs, spread, preferred_element_type=jnp.float32)
        for k in range(listed):
            span = pl.ds(pl.multiple_of(near_ref[t, k] * (3 * TILE), TILE), 3 * TILE)
            geos[s][k] = jnp.dot(lhs, right[:, span], preferred_element_type=jnp.float32)

    def blocks(t, s, selfs):
        own = first_tile + t
        own_span = pl.ds(pl.multiple_of(own * TILE, TILE), TILE)
        near = [near_ref[t, k] for k in range(listed)]
        near_spans = [pl.ds(pl.multiple_of(n * TILE, TILE), TILE) for n in near]
        twice = jnp.float32(0.0)
        for n in near:
            twice = twice + (n == own).astype(jnp.float32)
        mine = cols[:, own_span]
        selfs = selfs + twice * (mine * mine)
        for b in range(TILE // SUB):
            rows = pl.ds(b * SUB, SUB)
            qi = owns[s][rows, 0:TILE]
            e6 = owns[s][rows, TILE : 2 * TILE]
            sums = [None] * 10

            def put(slot, value):
                sums[slot] = value if sums[slot] is None else sums[slot] + value

            for k, span in enumerate(near_spans):
                def col(c):
                    return jnp.broadcast_to(cols[c : c + 1, span], (SUB, TILE))

                inv = lax.rsqrt(geos[s][k, rows, 0:TILE])
                root = lax.rsqrt(geos[s][k, rows, TILE : 2 * TILE])
                p = root * root
                x = geos[s][k, rows, 2 * TILE : 3 * TILE] * p
                x3 = x * x * x
                low = x3 - 1.0
                lj = x3 * low
                charge = col(4) * inv
                put(4, charge)
                put(5, col(5) * lj)
                put(6, col(6) * inv)
                put(7, col(7) * lj)
                put(8, col(8) * inv)
                put(9, col(9) * lj)
                w = qi * (charge * (inv * inv)) + (e6 * col(5)) * ((x3 * p) * (x3 + low))
                put(0, w * col(0))
                put(1, w * col(1))
                put(2, w * col(2))
                put(3, w)
            for c in range(10):
                accs[s][c, rows, :] = sums[c]
        return selfs

    def finish(t, s, totals):
        own_span = pl.ds(pl.multiple_of((first_tile + t) * TILE, TILE), TILE)
        flat = []
        for c in range(0, 10, 2):
            pair = []
            for whole in (accs[s][c], accs[s][c + 1]):
                high = whole.astype(jnp.bfloat16)
                rest = (whole - high.astype(jnp.float32)).astype(jnp.bfloat16)
                pair.append(jnp.concatenate([high, rest], axis=1))
            both = lane_sums(ones, jnp.concatenate(pair, axis=0))
            flat += [both[0:1, :TILE], both[0:1, TILE:]]
        mine = cols[:, own_span]
        out_span = pl.ds(pl.multiple_of(t * TILE, TILE), TILE)
        for c in range(3):
            force_ref[0, c : c + 1, out_span] = mine[c : c + 1] * flat[3] - flat[c]
        return tuple(
            totals[h]
            + (mine[4 + 2 * h : 5 + 2 * h] * flat[4 + 2 * h] + mine[5 + 2 * h : 6 + 2 * h] * flat[5 + 2 * h])
            for h in range(3)
        )

    def two_tiles(m, carry):
        totals, selfs = carry
        t = 2 * m
        totals = finish(jnp.maximum(t - 1, 0), 1, totals)
        geometry(t + 1, 1)
        selfs = blocks(t, 0, selfs)
        totals = finish(t, 0, totals)
        geometry(jnp.minimum(t + 2, row_tiles - 1), 0)
        selfs = blocks(t + 1, 1, selfs)
        return totals, selfs

    zero = jnp.zeros((16, TILE), jnp.float32)
    none = jnp.zeros((1, TILE), jnp.float32)
    accs[1][...] = jnp.zeros(accs[1].shape, jnp.float32)
    geometry(0, 0)
    totals, selfs = lax.fori_loop(0, row_tiles // 2, two_tiles, ((none,) * 3, zero))
    totals = finish(row_tiles - 1, 1, totals)
    soft = lax.rsqrt(jnp.full((1, TILE), DELTA_SOFT, jnp.float32))
    lane1 = lax.broadcasted_iota(jnp.int32, (1, TILE), 1)
    line = jnp.zeros((1, TILE), jnp.float32)
    for h in range(3):
        c = 4 + 2 * h
        value = jnp.sum(totals[h] - selfs[c : c + 1] * soft)
        line = jnp.where(lane1 == h, value, line)
    energy_ref[...] = line


def per_device(
    coords, velocities, coupling, charges, types, type_sigma, type_eps, near_tiles, accept
):
    parts, width = lax.axis_size("atom"), coords.shape[2]
    atoms = parts * width
    part = lax.axis_index("atom")
    packed = jnp.concatenate([coords, velocities, coupling], axis=1)
    rows = jnp.concatenate([coords, coupling], axis=1)
    lower, upper = moved(packed, 1, 0), moved(packed, -1, 0)
    halves = [rows] + [moved(rows, 0, step) for step in range(1, parts)]
    for by, block in ((1, lower), (-1, upper)):
        halves.append(block)
        for step in range(1, parts):
            halves.append(moved(coupling, by, step))

    smem = pl.BlockSpec(memory_space=pltpu.SMEM)
    vmem = pl.BlockSpec(memory_space=pltpu.VMEM)
    pairs = width * near_tiles.shape[1] * TILE
    force, line = pl.pallas_call(
        partial(tiles_kernel, parts, near_tiles.shape[1]),
        out_shape=(
            jax.ShapeDtypeStruct(coords.shape, jnp.float32),
            jax.ShapeDtypeStruct((1, TILE), jnp.float32),
        ),
        in_specs=[smem] * 4 + [vmem] * (2 + len(halves)),
        out_specs=(vmem, vmem),
        scratch_shapes=[
            pltpu.VMEM((16, atoms), jnp.float32),
            pltpu.VMEM((DEPTH, atoms), jnp.float32),
            pltpu.VMEM((DEPTH, 3 * atoms), jnp.bfloat16),
            pltpu.VMEM((DEPTH, 4 * TILE), jnp.float32),
            pltpu.VMEM((DEPTH, 4 * TILE), jnp.float32),
        ]
        + [pltpu.VMEM((near_tiles.shape[1], TILE, 3 * TILE), jnp.float32)] * 2
        + [pltpu.VMEM((TILE, 2 * TILE), jnp.float32)] * 2
        + [pltpu.VMEM((10, TILE, TILE), jnp.float32)] * 2,
        cost_estimate=pl.CostEstimate(
            flops=50 * pairs, bytes_accessed=4 * 20 * atoms, transcendentals=2 * pairs
        ),
        name="tiles",
    )(
        part.reshape(1).astype(jnp.int32),
        near_tiles,
        type_sigma,
        type_eps,
        charges.reshape(1, atoms),
        types.reshape(1, atoms),
        *halves,
    )
    shares = jnp.stack([line[0, :3]] + [moved(line, 0, step)[0, :3] for step in range(1, parts)])
    total = shares[0]
    for step in range(1, parts):
        total = total + shares[step]
    if parts > 2:
        order = (jnp.arange(parts) - part) % parts
        total = jnp.sum(shares[order], axis=0)
    energies = (total * (0.5 / atoms))[None]

    replica, cycle = lax.axis_index("lam"), lax.axis_size("lam")
    up = accept[replica] == 1
    low = accept[(replica + cycle - 1) % cycle] == 1
    new_coords = jnp.where(up, upper[:, 0:3], jnp.where(low, lower[:, 0:3], coords))
    new_velocities = jnp.where(up, upper[:, 3:6], jnp.where(low, lower[:, 3:6], velocities))
    return (energies, force, new_coords, new_velocities)


def solution(mesh):
    split = P("lam", None, "atom")
    return jax.shard_map(
        per_device,
        mesh=mesh,
        in_specs=(split, split, split, P(), P(), P(), P(), P("atom", None), P()),
        out_specs=(P("lam", None), split, split, split),
        check_vma=False,
    )
```
